256 devices in a mesh: gx: 16 (over x, z_lo, core), gy: 16 (over y, z_hi).
Axes of the slice: x: 4, y: 4, z: 8 (z_hi: 4, z_lo: 2; z = z_hi * 2 + z_lo), core: 2. Of those that a mesh axis runs over, the one named last changes fastest.
Arguments:
- tokens: bfloat16 [131072, 1280], P(('gx', 'gy')), may hold values from -6 to 6
- out_grad: bfloat16 [131072, 1280], P(('gx', 'gy')), may hold values from -400 to 400
- segments: int32 [256, 512], P(('gx', 'gy')), may hold values from 0 to 7, never falling along the last dimension, each value on 1 to 256 neighbouring positions
- pos_rows: int32 [131072], P(('gx', 'gy')), may hold values from 0 to 15
- pos_cols: int32 [131072], P(('gx', 'gy')), may hold values from 0 to 15
- row_table: bfloat16 [16, 1280], replicated, may hold values from -4 to 4
- col_table: bfloat16 [16, 1280], replicated, may hold values from -4 to 4
- norm_gain: float32 [1280], replicated, may hold values from 0.25 to 1.75
- master_up: float32 [1280, 2560], P('gx'), may hold values from -0.15625 to 0.15625
- master_down: float32 [1280, 2560], P('gx'), may hold values from -0.125 to 0.125
- moment_up: float32 [1280, 2560], P('gx'), may hold values from -6 to 6
- moment_down: float32 [1280, 2560], P('gx'), may hold values from -6 to 6
Outputs:
- new_master_up: float32 [1280, 2560], P('gx')
- new_master_down: float32 [1280, 2560], P('gx')
- new_moment_up: float32 [1280, 2560], P('gx')
- new_moment_down: float32 [1280, 2560], P('gx')
The draws below stay inside these ranges and needn't reach their ends.
Inputs may be any that keep to these rules, and one draw needn't show every extreme that they name: `segments`: each replica's 512 tokens hold all 8 images in order, each of 1 to 256 tokens.
All inputs are finite; a program needn't handle non-finite values.
Results may differ from the reference program's by a relative error of at most 0.02.
Values may be sent and summed in bfloat16 or wider, within the bound.
No kernel may reach another device: no remote copies, remote signals or barrier semaphores. Data moves between devices by JAX's collectives and lax.ppermute only.
A program may use at most 128 MiB of HBM per device.

```python
import math
import jax
import jax.numpy as jnp
import numpy as np
from jax import lax

D = 1280
FF = 2560
GRID = 16
IMGS = 8
TOK_DEV = 512
MOST = 256
TOKENS = 131072
N_GX = 16
N_GY = 16
DEVICES = 256


def draw_out_grad(key, part):
    first_key, second_key = jax.random.split(key, 2)
    feature = jnp.arange(D, dtype=jnp.float32) / D
    roughness = jax.random.uniform(second_key, (D,), minval=0.5, maxval=2.0)
    base = jnp.clip(jax.random.normal(first_key, (TOKENS, D)), -5.0, 5.0)
    rising = jnp.exp(jnp.log(3.0) * feature)
    values = base * rising[None, :] * roughness[None, :]
    return values.astype(jnp.bfloat16)


def set_ends(result, stream_key, low, high):
    place = [jax.random.randint(jax.random.fold_in(stream_key, axis), (), 0, length) for axis, length in enumerate(result.shape)]
    longest = result.shape.index(max(result.shape))
    neighbour = place[:longest] + [(place[longest] + 1) % result.shape[longest]] + place[longest + 1:]
    return result.at[tuple(place)].set(low).at[tuple(neighbour)].set(high)


def block_levels(stream_key, dims, cuts, least, largest):
    loudness = 1.0
    for axis_at, parts in cuts:
        heights = jax.random.uniform(jax.random.fold_in(jax.random.fold_in(stream_key, 6), axis_at), (parts,), jnp.float32, least / len(cuts), largest / len(cuts))
        loudness = loudness * jnp.repeat(jnp.exp(heights), dims[axis_at] // parts).reshape((-1,) + (1,) * (len(dims) - 1 - axis_at))
    return loudness


def split_up(number_of, total, reach, slope):
    weights = [(1 << 20) // math.isqrt(grade ** slope) + 1 for grade in range(2, number_of + 1)]
    spare, counts = total - reach - (number_of - 1), [1] * (number_of - 1)
    while spare > 0:
        candidates = [i for i in range(number_of - 1) if counts[i] < reach]
        whole, left = sum([weights[i] for i in candidates]), spare
        for i in candidates:
            extra = min(reach - counts[i], max(1, left * weights[i] // whole), spare)
            counts[i] = counts[i] + extra
            spare = spare - extra
    return np.array([reach] + counts)


def uneven_parts(key, number_of, total, limit, lean):
    if number_of == 2:
        one = jax.random.randint(key, (), max(1, total - limit), min(limit, total - 1) + 1)
        return jnp.stack([one, total - one])
    tallies = jnp.asarray(split_up(number_of, total, limit, lean), jnp.int32)
    twos = (number_of - 1) // 2
    donor, taker = tallies[1:1 + 2 * twos:2], tallies[2:2 + 2 * twos:2]
    margin = jnp.minimum(donor - 1, limit - taker)
    passed = jax.random.randint(jax.random.fold_in(key, 1), (twos,), 0, 1 << 20) % (margin + 1)
    tallies = tallies.at[1:1 + 2 * twos:2].set(donor - passed).at[2:2 + 2 * twos:2].set(taker + passed)
    return tallies[jax.random.permutation(jax.random.fold_in(key, 2), number_of)]


def bell_draw(key, dims, spread, most, cuts=(), kind=jnp.bfloat16):
    values = spread * jax.random.normal(key, dims, jnp.float32)
    if cuts:
        values = values * block_levels(key, dims, cuts, -0.22, 0.18)
    return jnp.clip(values, -most, most).astype(kind)


def setup_inputs(seed: int = 0) -> dict:
    key_of = jax.random.split(jax.random.key(seed), 13)
    return {
        "tokens": bell_draw(key_of[0], (TOKENS, D), 1.0, 6.0, ((0, 256),)),
        "out_grad": draw_out_grad(jax.random.fold_in(key_of[12], 71), 0),
        "segments": jax.vmap(lambda own: jnp.searchsorted(jnp.cumsum(uneven_parts(own, IMGS, TOK_DEV, MOST, 2)), jnp.arange(TOK_DEV), side="right"))(jax.random.split(key_of[2], DEVICES)).reshape((DEVICES, TOK_DEV)).astype(jnp.int32),
        "pos_rows": set_ends(jax.random.randint(key_of[3], (TOKENS,), 0, GRID), jax.random.fold_in(key_of[3], 1), 0, GRID - 1).astype(jnp.int32),
        "pos_cols": set_ends(jax.random.randint(key_of[4], (TOKENS,), 0, GRID), jax.random.fold_in(key_of[4], 1), 0, GRID - 1).astype(jnp.int32),
        "row_table": bell_draw(key_of[5], (GRID, D), 0.7, 4.0),
        "col_table": bell_draw(key_of[6], (GRID, D), 0.7, 4.0),
        "norm_gain": jnp.clip(1.0 + 0.15 * jax.random.normal(key_of[7], (D,), jnp.float32), 0.25, 1.75),
        "master_up": bell_draw(key_of[8], (D, FF), D ** -0.5, 0.15625, ((0, 16),), jnp.float32),
        "master_down": bell_draw(key_of[9], (D, FF), FF ** -0.5, 0.125, ((0, 16),), jnp.float32),
        "moment_up": bell_draw(key_of[10], (D, FF), 1.0, 6.0, ((0, 16),), jnp.float32),
        "moment_down": bell_draw(key_of[11], (D, FF), 1.0, 6.0, ((0, 16),), jnp.float32),
    }


momentum_keep = 0.9
learn_rate = 0.01

def gelu_tanh(values):
    return 0.5 * values * (1.0 + jnp.tanh(0.7978845608 * (values + 0.044715 * values * values * values)))

def table_lookup(positions, table):
    onehot = (positions[:, None] == jnp.arange(GRID, dtype=jnp.int32)[None, :]).astype(jnp.bfloat16)
    return jnp.dot(onehot, table, preferred_element_type=jnp.float32)

def replica_grads(tok_rows, grad_rows, seg_row, row_ids, col_ids, row_table, col_table, norm_gain, w_up, w_down):
    embedded = tok_rows.astype(jnp.float32) + table_lookup(row_ids, row_table) + table_lookup(col_ids, col_table)
    average = lax.optimization_barrier(jnp.mean(embedded, axis=1, keepdims=True))
    centered = embedded - average
    variance = lax.optimization_barrier(jnp.mean(centered * centered, axis=1, keepdims=True))
    normed = (centered * lax.rsqrt(variance + 1e-06) * norm_gain[None, :]).astype(jnp.bfloat16)
    pre_act = jnp.dot(normed, w_up, preferred_element_type=jnp.float32)
    hidden = gelu_tanh(pre_act).astype(jnp.bfloat16)
    member = (seg_row[:, None] == jnp.arange(IMGS, dtype=jnp.int32)[None, :]).astype(jnp.float32)
    per_image = 1.0 / lax.optimization_barrier(jnp.sum(member, axis=0))
    token_weight = jnp.dot(member, per_image)
    weighted = (grad_rows.astype(jnp.float32) * token_weight[:, None]).astype(jnp.bfloat16)
    hidden_grad = jnp.dot(weighted, w_down, preferred_element_type=jnp.float32)
    _, backward = jax.vjp(gelu_tanh, pre_act)
    pre_grad = backward(hidden_grad)[0].astype(jnp.bfloat16)
    grad_up = lax.dot_general(normed, pre_grad, (((0,), (0,)), ((), ())), preferred_element_type=jnp.float32)
    grad_down = lax.dot_general(weighted, hidden, (((0,), (0,)), ((), ())), preferred_element_type=jnp.float32)
    return jnp.concatenate([grad_up.astype(jnp.bfloat16), grad_down.astype(jnp.bfloat16)], axis=1)

def reference(tokens, out_grad, segments, pos_rows, pos_cols, row_table, col_table, norm_gain, master_up, master_down, moment_up, moment_down):
    w_up = master_up.astype(jnp.bfloat16)
    w_down = master_down.astype(jnp.bfloat16)
    replicas = N_GX * N_GY

    def accumulate(running, replica):
        first = (replica * TOK_DEV).astype(jnp.int32)
        tok_rows = lax.dynamic_slice_in_dim(tokens, first, TOK_DEV, 0)
        grad_rows = lax.dynamic_slice_in_dim(out_grad, first, TOK_DEV, 0)
        row_ids = lax.dynamic_slice_in_dim(pos_rows, first, TOK_DEV, 0)
        col_ids = lax.dynamic_slice_in_dim(pos_cols, first, TOK_DEV, 0)
        seg_row = lax.dynamic_slice_in_dim(segments, replica.astype(jnp.int32), 1, 0)[0]
        grads = replica_grads(tok_rows, grad_rows, seg_row, row_ids, col_ids, row_table, col_table, norm_gain, w_up, w_down)
        return (running + grads.astype(jnp.float32), None)
    start_sum = jnp.zeros((D, 2 * FF), jnp.float32)
    grad_sum, _ = lax.scan(accumulate, start_sum, jnp.arange(replicas, dtype=jnp.int32))
    scale = lax.rsqrt(jnp.mean(grad_sum * grad_sum) + 1e-06)
    moments = jnp.concatenate([moment_up, moment_down], axis=1)
    masters = jnp.concatenate([master_up, master_down], axis=1)
    new_moments = momentum_keep * moments + scale * grad_sum
    new_masters = masters - learn_rate * new_moments
    return (new_masters[:, :FF], new_masters[:, FF:], new_moments[:, :FF], new_moments[:, FF:])
```

```python
import jax
import jax.numpy as jnp
from jax import lax
from jax.sharding import Mesh
from jax.sharding import PartitionSpec as P

D = 1280
FF = 2560
GRID = 16
IMGS = 8
HALF = 1280
HX = 768
HY = HALF - HX
BLK = 40
GX = ("x", "zl", "c")
GX_GY = ("x", "zl", "c", "y", "zh")
BF = jnp.bfloat16
F32 = jnp.float32

momentum_keep = 0.9
learn_rate = 0.01


def ring(value, axis, step):
    return lax.ppermute(value, axis, [(i, (i + step) % 4) for i in range(4)])


def swap(value, axis):
    return lax.ppermute(value, axis, [(0, 1), (1, 0)])


def z_ring(value, step):
    at = lambda z: (z % 2) * 4 + z // 2
    return lax.ppermute(value, ("zl", "zh"), [(at(z), at((z + step) % 8)) for z in range(8)])


def ring_gather(piece, axis):
    h = piece.shape[0] // 2
    before = ring(piece, axis, 1)
    after = ring(piece, axis, -1)
    far_a = ring(before[:h], axis, 1)
    far_b = ring(after[h:], axis, -1)
    return jnp.concatenate([piece, after, far_a, far_b, before], axis=0)


def ring_scatter(up, down, axis):
    rows = up.shape[0] // 4
    u = [up[k * rows : (k + 1) * rows] for k in range(4)]
    d = [down[k * rows : (k + 1) * rows] for k in range(4)]
    a = ring(jnp.stack([u[2], d[1]]), axis, 1)
    b = ring(jnp.stack([d[2], u[3]]), axis, -1)
    c = ring((u[1].astype(F32) + a[0].astype(F32)).astype(BF), axis, 1)
    e = ring((d[3].astype(F32) + b[0].astype(F32)).astype(BF), axis, -1)
    own_u = u[0].astype(F32) + c.astype(F32) + b[1].astype(F32)
    own_d = d[0].astype(F32) + a[1].astype(F32) + e.astype(F32)
    return jnp.concatenate([own_u, own_d], axis=1).astype(BF)


def direct_scatter(q, axis):
    r1 = ring(q[1], axis, 1)
    r3 = ring(q[3], axis, -1)
    r2 = ring(q[2], axis, 2)
    return q[0].astype(F32) + r1.astype(F32) + r2.astype(F32) + r3.astype(F32)


def direct_gather(piece, axis, index):
    before = ring(piece, axis, 1)
    after = ring(piece, axis, -1)
    far = ring(piece, axis, 2)
    relative = jnp.stack([piece, after, far, before])
    return rolled(relative, (4 - index) % 4)


def rolled(blocks, start):
    n = blocks.shape[0]
    return lax.dynamic_slice_in_dim(jnp.concatenate([blocks, blocks], axis=0), start, n, 0)


def direct_sum(value, axis):
    return value + ring(value, axis, 1) + ring(value, axis, -1) + ring(value, axis, 2)


def gelu_and_slope(v):
    t = jnp.tanh(0.7978845608 * (v + 0.044715 * v * v * v))
    half = 0.5 * (1.0 + t)
    slope = half + 0.5 * v * (1.0 - t * t) * (0.7978845608 * (1.0 + 0.134145 * v * v))
    return v * half, slope


def table_lookup(positions, table):
    onehot = (positions[:, None] == jnp.arange(GRID, dtype=jnp.int32)[None, :]).astype(BF)
    return jnp.dot(onehot, table, preferred_element_type=F32)


def column_product(left, right):
    return lax.dot_general(
        left, right, (((0,), (0,)), ((), ())), preferred_element_type=F32
    ).astype(BF)


def on_device(
    tokens,
    out_grad,
    segments,
    pos_rows,
    pos_cols,
    row_table,
    col_table,
    norm_gain,
    master_up,
    master_down,
    moment_up,
    moment_down,
):
    ix, iz, ic = lax.axis_index("x"), lax.axis_index("zl"), lax.axis_index("c")
    iy, ih = lax.axis_index("y"), lax.axis_index("zh")
    low_core = ic == 0

    up, down = master_up.astype(BF), master_down.astype(BF)

    def columns(k):
        u, d = up[:, k * HALF : (k + 1) * HALF], down[:, k * HALF : (k + 1) * HALF]
        return jnp.concatenate([u[:, :HX], d[:, :HX], u[:, HX:], d[:, HX:]], axis=1)

    lo, hi = columns(0), columns(1)
    mine = jnp.where(low_core, lo, hi)
    other = swap(jnp.where(low_core, hi, lo), "c")
    rows = jnp.concatenate(
        [jnp.where(low_core, mine, other), jnp.where(low_core, other, mine)], axis=0
    )
    rows = rolled(rows.reshape(4, BLK, 2 * HALF), iy).reshape(4 * BLK, 2 * HALF)

    vy = rows[:BLK, 2 * HX :]
    vy_other = jnp.concatenate([z_ring(vy[:, :HY], 1), z_ring(vy[:, HY:], -1)], axis=1)
    wy = ring_gather(ring_gather(jnp.concatenate([vy, vy_other], axis=0), "x"), "y")
    vx = rows[:, : 2 * HX]
    vx_other = [z_ring(vx[: 2 * BLK], 1), z_ring(vx[2 * BLK :], -1)]
    wx = ring_gather(jnp.concatenate([vx, *vx_other], axis=0), "x")

    embedded = (
        tokens.astype(F32) + table_lookup(pos_rows, row_table) + table_lookup(pos_cols, col_table)
    )
    average = jnp.mean(embedded, axis=1, keepdims=True)
    centered = embedded - average
    variance = jnp.mean(centered * centered, axis=1, keepdims=True)
    normed = (centered * lax.rsqrt(variance + 1e-06) * norm_gain[None, :]).astype(BF)
    member = (segments[0][:, None] == jnp.arange(IMGS, dtype=jnp.int32)[None, :]).astype(F32)
    per_image = 1.0 / jnp.sum(member, axis=0)
    token_weight = jnp.sum(member * per_image[None, :], axis=1)
    weighted = (out_grad.astype(F32) * token_weight[:, None]).astype(BF)

    place = jnp.arange(D, dtype=jnp.int32)
    block, within = place // BLK, place % BLK

    def source(dx, dz, dy):
        return (((ix + dx) % 4 * 2 + (iz + dz) % 2) * 4 + (iy + dy) % 4) * BLK + within

    from_x = source(block // 8, block // 4 % 2, block % 4)
    from_y = source(block // 2 % 4, block % 2, block // 8)

    def turned(values, source_of):
        onehot = (place[:, None] == source_of[None, :]).astype(BF)
        own = jnp.dot(values, onehot, preferred_element_type=F32).astype(BF)
        return jnp.concatenate([own, swap(own, "c")], axis=0)

    def gradients(w, h, source_of, axis):
        left, right = turned(normed, source_of), turned(weighted, source_of)
        pre_act = jnp.dot(left, w[:, :h], preferred_element_type=F32)
        hidden_grad = jnp.dot(right, w[:, h:], preferred_element_type=F32)
        hidden, slope = gelu_and_slope(pre_act)
        pre_grad = (hidden_grad * slope).astype(BF)
        return ring_scatter(
            column_product(left, pre_grad), column_product(right, hidden.astype(BF)), axis
        )

    sx = gradients(wx, HX, from_x, "x").reshape(2, 4, BLK, 2 * HX)
    sy = gradients(wy, HY, from_y, "y").reshape(4, 2 * BLK, 2 * HY)
    sx = direct_scatter([sx[:, k].reshape(2 * BLK, 2 * HX) for k in range(4)], "y")
    sy = direct_scatter([sy[k] for k in range(4)], "x")
    both = jnp.concatenate([sx, sy], axis=1)
    both = both[:BLK] + swap(both[BLK:].astype(BF), "zl").astype(F32)
    parts = jnp.stack([both[:, k * 640 : (k + 1) * 640] for k in range(4)]).astype(BF)
    parts = rolled(parts, ih)
    share = direct_scatter([parts[k] for k in range(4)], "zh").astype(BF)

    gathered = direct_gather(share, "zh", ih)
    gathered = jnp.concatenate([gathered[k] for k in range(4)], axis=1)
    wide = gathered.astype(F32)
    squares = jnp.full((8, 128), jnp.sum(wide * wide), F32)
    squares = direct_sum(squares, "x")
    squares = squares + swap(squares, "zl")
    squares = squares + swap(squares, "c")
    squares = direct_sum(squares, "y")
    scale = lax.rsqrt(squares[:1, :1] / (2.0 * D * FF) + 1e-06)

    rows_of = direct_gather(gathered, "y", iy).reshape(4 * BLK, 2 * HALF)
    first, last = rows_of[: 2 * BLK], rows_of[2 * BLK :]
    keep = jnp.where(low_core, first, last)
    got = swap(jnp.where(low_core, last, first), "c")
    lo, hi = jnp.where(low_core, keep, got), jnp.where(low_core, got, keep)

    def updated(start_x, start_y, master, moment):
        grad = jnp.concatenate(
            [
                part
                for half in (lo, hi)
                for part in (half[:, start_x : start_x + HX], half[:, start_y : start_y + HY])
            ],
            axis=1,
        ).astype(F32)
        new_moment = momentum_keep * moment + scale * grad
        return master - learn_rate * new_moment, new_moment

    new_up, new_moment_up = updated(0, 2 * HX, master_up, moment_up)
    new_down, new_moment_down = updated(HX, 2 * HX + HY, master_down, moment_down)
    return new_up, new_down, new_moment_up, new_moment_down


def solution(mesh):
    split = Mesh(mesh.devices.reshape(4, 2, 2, 4, 4), ("x", "zl", "c", "y", "zh"))
    return jax.shard_map(
        on_device,
        mesh=split,
        in_specs=(
            P(GX_GY, None),
            P(GX_GY, None),
            P(GX_GY, None),
            P(GX_GY),
            P(GX_GY),
            P(),
            P(),
            P(),
            P(GX, None),
            P(GX, None),
            P(GX, None),
            P(GX, None),
        ),
        out_specs=(P(GX, None), P(GX, None), P(GX, None), P(GX, None)),
        check_vma=False,
    )
```

```python
import jax
import jax.numpy as jnp
from jax import lax
from jax.experimental import pallas as pl
from jax.experimental.pallas import tpu as pltpu
from jax.sharding import Mesh
from jax.sharding import PartitionSpec as P

D = 1280
FF = 2560
GRID = 16
IMGS = 8
HALF = 1280
HX = 768
HY = HALF - HX
BLK = 40
GX = ("x", "zl", "c")
GX_GY = ("x", "zl", "c", "y", "zh")
BF = jnp.bfloat16
F32 = jnp.float32

momentum_keep = 0.9
learn_rate = 0.01


def ring(value, axis, step):
    return lax.ppermute(value, axis, [(i, (i + step) % 4) for i in range(4)])


def swap(value, axis):
    return lax.ppermute(value, axis, [(0, 1), (1, 0)])


def z_ring(value, step):
    at = lambda z: (z % 2) * 4 + z // 2
    return lax.ppermute(value, ("zl", "zh"), [(at(z), at((z + step) % 8)) for z in range(8)])


def ring_gather(piece, axis):
    h = piece.shape[0] // 2
    before = ring(piece, axis, 1)
    after = ring(piece, axis, -1)
    far_a = ring(before[:h], axis, 1)
    far_b = ring(after[h:], axis, -1)
    return [piece, after, far_a, far_b, before]


def ring_scatter(plus, minus, mid, own, axis):
    a = ring(plus, axis, 1)
    b = ring(minus, axis, -1)
    c = ring((mid[0].astype(F32) + a[0].astype(F32)).astype(BF), axis, 1)
    e = ring((mid[1].astype(F32) + b[0].astype(F32)).astype(BF), axis, -1)
    own_u = own[0].astype(F32) + c.astype(F32) + b[1].astype(F32)
    own_d = own[1].astype(F32) + a[1].astype(F32) + e.astype(F32)
    return jnp.concatenate([own_u, own_d], axis=1).astype(BF)


def direct_scatter(q, axis):
    r1 = ring(q[1], axis, 1)
    r3 = ring(q[3], axis, -1)
    r2 = ring(q[2], axis, 2)
    return q[0].astype(F32) + r1.astype(F32) + r2.astype(F32) + r3.astype(F32)


def direct_gather(piece, axis, index):
    before = ring(piece, axis, 1)
    after = ring(piece, axis, -1)
    far = ring(piece, axis, 2)
    relative = jnp.stack([piece, after, far, before])
    return rolled(relative, (4 - index) % 4)


def rolled(blocks, start):
    n = blocks.shape[0]
    return lax.dynamic_slice_in_dim(jnp.concatenate([blocks, blocks], axis=0), start, n, 0)


def direct_sum(value, axis):
    return value + ring(value, axis, 1) + ring(value, axis, -1) + ring(value, axis, 2)


def gelu_and_slope(v):
    t = jnp.tanh(0.7978845608 * (v + 0.044715 * v * v * v))
    half = 0.5 * (1.0 + t)
    slope = half + 0.5 * v * (1.0 - t * t) * (0.7978845608 * (1.0 + 0.134145 * v * v))
    return v * half, slope


def dot(left, right):
    return jnp.dot(left, right, preferred_element_type=F32)


def gradients_kernel(by_y, tok_refs, pieces, outs, scratch):
    plus, minus, mid, own = outs
    wu, wd, pg, hd, rows_in, columns_in, arrived = scratch
    copies = [
        pltpu.make_async_copy(
            ref, rows_in.at[i] if i < 4 else columns_in.at[i - 4], arrived.at[i]
        )
        for i, ref in enumerate(tok_refs)
    ]
    n, w = (rows_in.at[0], rows_in.at[1]), (rows_in.at[2], rows_in.at[3])
    nt, wt = (columns_in.at[0], columns_in.at[1]), (columns_in.at[2], columns_in.at[3])

    @pl.when(pl.program_id(0) == 0)
    def _():
        for copy in copies:
            copy.start()

    count = len(pieces) // 2
    for group, whole in ((pieces[:count], wu), (pieces[count:], wd)):
        start = 0
        for piece in group:
            size = piece.shape[0]
            if by_y:
                for j in range(0, size, BLK):
                    dy, chunk = divmod((start + j) // BLK, 8)
                    at = (chunk * 4 + dy) * BLK
                    whole[at : at + BLK, :] = piece[j : j + BLK, :]
            else:
                whole[start : start + size, :] = piece[...]
            start += size

    @pl.when(pl.program_id(0) == 0)
    def _():
        for copy in copies[:4]:
            copy.wait()

    half = n[0].shape[0]
    for core in range(2):
        for m in range(0, half, 256):
            v = dot(n[core][m : m + 256, :], wu[...])
            hidden_grad = dot(w[core][m : m + 256, :], wd[...])
            hidden, slope = gelu_and_slope(v)
            at = core * half + m
            hd[at : at + 256, :] = hidden.astype(BF)
            pg[at : at + 256, :] = (hidden_grad * slope).astype(BF)

    @pl.when(pl.program_id(0) == 0)
    def _():
        for copy in copies[4:]:
            copy.wait()

    q = D // 4
    up_to = ((own, 0), (mid, 0), (plus, 0), (minus, 1))
    down_to = ((own, 1), (plus, 1), (minus, 0), (mid, 1))
    for k in (2, 1, 3, 0):
        rows = slice(k * q, (k + 1) * q)
        for left, right, to in ((nt, pg, up_to), (wt, hd, down_to)):
            grad = dot(left[0][rows, :], right[:half, :]) + dot(left[1][rows, :], right[half:, :])
            if by_y:
                for j in range(8):
                    dz, dy = divmod(j, 4)
                    out, slot = to[dy]
                    at = (k * 2 + dz) * BLK
                    out[slot, at : at + BLK, :] = grad[j * BLK : (j + 1) * BLK, :].astype(BF)
            else:
                out, slot = to[k]
                out[slot] = grad.astype(BF)


def gradients(pieces, features, by_y):
    h = pieces[0].shape[1] // 2
    tokens = 2 * features[0].shape[0]
    blocks = h // 256
    count = len(pieces)

    def body(*refs):
        tok_refs, refs = refs[:8], refs[8:]
        gradients_kernel(
            by_y, tok_refs, refs[: 2 * count], refs[2 * count : 2 * count + 4], refs[-7:]
        )

    at = lambda first: [
        pl.BlockSpec((p.shape[0], 256), lambda n, first=first: (0, n + first)) for p in pieces
    ]
    q = D // 4
    return pl.pallas_call(
        body,
        grid=(blocks,),
        in_specs=[pl.BlockSpec(memory_space=pl.ANY)] * 8 + at(0) + at(blocks),
        out_specs=[pl.BlockSpec((2, q, 256), lambda n: (0, 0, n))] * 4,
        out_shape=[jax.ShapeDtypeStruct((2, q, h), BF)] * 4,
        scratch_shapes=[pltpu.VMEM((D, 256), BF)] * 2
        + [pltpu.VMEM((tokens, 256), BF)] * 2
        + [pltpu.VMEM((4, tokens // 2, D), BF), pltpu.VMEM((4, D, tokens // 2), BF)]
        + [pltpu.SemaphoreType.DMA((8,))],
        compiler_params=pltpu.CompilerParams(vmem_limit_bytes=30 * 1024 * 1024),
        cost_estimate=pl.CostEstimate(
            flops=8 * tokens * D * h,
            bytes_accessed=2 * (4 * tokens * D + 4 * D * h),
            transcendentals=tokens * h,
        ),
        name="gradients_y" if by_y else "gradients_x",
    )(*features, *pieces, *pieces)


def turn_kernel(source, values, others, n, w, nt, wt):
    row = lax.broadcasted_iota(jnp.int32, (D, 256), 0)
    onehot = jnp.where(row == source[...], 1.0, 0.0).astype(BF)
    for left, out, out_t in ((values, n, nt), (others, w, wt)):
        turned = dot(left[...], onehot)
        out[...] = turned.astype(BF)
        out_t[...] = turned.T.astype(BF)


def turned(source, values, others):
    tokens = values.shape[0]
    whole = pl.BlockSpec((tokens, D), lambda n: (0, 0))
    rows = pl.BlockSpec((tokens, 256), lambda n: (0, n))
    columns = pl.BlockSpec((256, tokens), lambda n: (n, 0))
    return pl.pallas_call(
        turn_kernel,
        grid=(D // 256,),
        in_specs=[pl.BlockSpec((1, 256), lambda n: (0, n)), whole, whole],
        out_specs=[rows, rows, columns, columns],
        out_shape=[jax.ShapeDtypeStruct((tokens, D), BF)] * 2
        + [jax.ShapeDtypeStruct((D, tokens), BF)] * 2,
        compiler_params=pltpu.CompilerParams(vmem_limit_bytes=20 * 1024 * 1024),
        cost_estimate=pl.CostEstimate(
            flops=4 * tokens * D * D, bytes_accessed=12 * tokens * D, transcendentals=0
        ),
        name="turn",
    )(source, values, others)


def table_lookup(positions, table):
    onehot = (positions[:, None] == jnp.arange(GRID, dtype=jnp.int32)[None, :]).astype(BF)
    return jnp.dot(onehot, table, preferred_element_type=F32)


def on_device(
    tokens,
    out_grad,
    segments,
    pos_rows,
    pos_cols,
    row_table,
    col_table,
    norm_gain,
    master_up,
    master_down,
    moment_up,
    moment_down,
):
    ix, iz, ic = lax.axis_index("x"), lax.axis_index("zl"), lax.axis_index("c")
    iy, ih = lax.axis_index("y"), lax.axis_index("zh")
    low_core = ic == 0

    up, down = master_up.astype(BF), master_down.astype(BF)

    def columns(k):
        u, d = up[:, k * HALF : (k + 1) * HALF], down[:, k * HALF : (k + 1) * HALF]
        return jnp.concatenate([u[:, :HX], d[:, :HX], u[:, HX:], d[:, HX:]], axis=1)

    lo, hi = columns(0), columns(1)
    mine = jnp.where(low_core, lo, hi)
    other = swap(jnp.where(low_core, hi, lo), "c")
    rows = jnp.concatenate(
        [jnp.where(low_core, mine, other), jnp.where(low_core, other, mine)], axis=0
    )
    rows = rolled(rows.reshape(4, BLK, 2 * HALF), iy).reshape(4 * BLK, 2 * HALF)

    tokens, out_grad, rows = lax.optimization_barrier((tokens, out_grad, rows))

    vx, vy = rows[:, : 2 * HX], rows[:BLK, 2 * HX :]

    def to_side(x_first, y_first):
        blocks = [vx[k * BLK : (k + 1) * BLK, x_first : x_first + HX] for k in range(4)]
        return jnp.concatenate([*blocks, vy[:, y_first : y_first + HY]], axis=1)

    low, high = z_ring(to_side(0, 0), 1), z_ring(to_side(HX, HY), -1)
    other_y = jnp.concatenate([low[:, 4 * HX :], high[:, 4 * HX :]], axis=1)
    other_x = [
        jnp.concatenate([part[:, k * HX : (k + 1) * HX] for part in (low, high)], axis=1)
        for k in range(4)
    ]
    wy = jnp.concatenate([vy, other_y], axis=0)
    before, after, far = ring(wy, "x", 1), ring(wy, "x", -1), ring(wy, "x", 2)
    wx = jnp.concatenate([vx, *other_x], axis=0)
    wx, before, after, far = lax.optimization_barrier((wx, before, after, far))
    wy = ring_gather(jnp.concatenate([wy, after, far, before], axis=0), "y")
    wx = ring_gather(wx, "x")

    embedded = (
        tokens.astype(F32) + table_lookup(pos_rows, row_table) + table_lookup(pos_cols, col_table)
    )
    average = jnp.mean(embedded, axis=1, keepdims=True)
    centered = embedded - average
    variance = jnp.mean(centered * centered, axis=1, keepdims=True)
    normed = (centered * lax.rsqrt(variance + 1e-06) * norm_gain[None, :]).astype(BF)
    member = (segments[0][:, None] == jnp.arange(IMGS, dtype=jnp.int32)[None, :]).astype(F32)
    per_image = 1.0 / jnp.sum(member, axis=0)
    token_weight = jnp.sum(member * per_image[None, :], axis=1)
    weighted = (out_grad.astype(F32) * token_weight[:, None]).astype(BF)

    place = jnp.arange(D, dtype=jnp.int32)
    block, within = place // BLK, place % BLK
    source = ((ix + block // 8) % 4 * 2 + (iz + block // 4 % 2) % 2) * 4 + (iy + block % 4) % 4
    features = []
    for own in turned((source * BLK + within)[None, :], normed, weighted):
        features += [own, swap(own, "c")]

    gy = gradients(wy, features, True)
    gx = gradients(wx, features, False)
    sx = ring_scatter(*gx, "x").reshape(2, 4, BLK, 2 * HX)
    sy = ring_scatter(*gy, "y").reshape(4, 2 * BLK, 2 * HY)
    sx = direct_scatter([sx[:, k].reshape(2 * BLK, 2 * HX) for k in range(4)], "y")
    sy = direct_scatter([sy[k] for k in range(4)], "x")
    both = jnp.concatenate([sx, sy], axis=1)
    both = both[:BLK] + swap(both[BLK:].astype(BF), "zl").astype(F32)
    parts = jnp.stack([both[:, k * 640 : (k + 1) * 640] for k in range(4)]).astype(BF)
    parts = rolled(parts, ih)
    share = direct_scatter([parts[k] for k in range(4)], "zh").astype(BF)

    gathered = direct_gather(share, "zh", ih)
    gathered = jnp.concatenate([gathered[k] for k in range(4)], axis=1)
    wide = gathered.astype(F32)
    squares = jnp.full((8, 128), jnp.sum(wide * wide), F32)
    squares = direct_sum(squares, "x")
    squares = squares + swap(squares, "zl")
    narrow = lambda value: lax.reduce_precision(value, 8, 7)
    second = squares - narrow(squares)
    third = second - narrow(second)
    row = lax.broadcasted_iota(jnp.int32, (8, 128), 0)
    terms = jnp.where(row == 0, squares, jnp.where(row == 1, second, jnp.where(row == 2, third, 0)))
    terms = jnp.broadcast_to(terms[:, :1], (8, 2 * HALF)).astype(BF)
    sent = jnp.concatenate([gathered, terms], axis=0)
    from_before, from_after, from_far = ring(sent, "y", 1), ring(sent, "y", -1), ring(sent, "y", 2)
    tail = lambda part: part[BLK:, :128].astype(F32)
    squares = terms[:, :128].astype(F32) + tail(from_before) + tail(from_after) + tail(from_far)
    squares = jnp.broadcast_to(jnp.sum(squares, axis=0, keepdims=True), (8, 128))
    squares = squares + swap(squares, "c")
    scale = lax.rsqrt(squares[:1, :1] / (2.0 * D * FF) + 1e-06)

    head = [part[:BLK] for part in (gathered, from_after, from_far, from_before)]
    rows_of = rolled(jnp.stack(head), (4 - iy) % 4).reshape(4 * BLK, 2 * HALF)
    first, last = rows_of[: 2 * BLK], rows_of[2 * BLK :]
    keep = jnp.where(low_core, first, last)
    got = swap(jnp.where(low_core, last, first), "c")
    lo, hi = jnp.where(low_core, keep, got), jnp.where(low_core, got, keep)

    def updated(start_x, start_y, master, moment):
        grad = jnp.concatenate(
            [
                part
                for half in (lo, hi)
                for part in (half[:, start_x : start_x + HX], half[:, start_y : start_y + HY])
            ],
            axis=1,
        ).astype(F32)
        new_moment = momentum_keep * moment + scale * grad
        return master - learn_rate * new_moment, new_moment

    new_up, new_moment_up = updated(0, 2 * HX, master_up, moment_up)
    new_down, new_moment_down = updated(HX, 2 * HX + HY, master_down, moment_down)
    return new_up, new_down, new_moment_up, new_moment_down


def solution(mesh):
    split = Mesh(mesh.devices.reshape(4, 2, 2, 4, 4), ("x", "zl", "c", "y", "zh"))
    return jax.shard_map(
        on_device,
        mesh=split,
        in_specs=(
            P(GX_GY, None),
            P(GX_GY, None),
            P(GX_GY, None),
            P(GX_GY),
            P(GX_GY),
            P(),
            P(),
            P(),
            P(GX, None),
            P(GX, None),
            P(GX, None),
            P(GX, None),
        ),
        out_specs=(P(GX, None), P(GX, None), P(GX, None), P(GX, None)),
        check_vma=False,
    )
```

```python
import jax
import jax.numpy as jnp
from jax import lax
from jax.experimental import pallas as pl
from jax.experimental.pallas import tpu as pltpu
from jax.sharding import Mesh
from jax.sharding import PartitionSpec as P

D = 1280
FF = 2560
GRID = 16
IMGS = 8
HALF = 1280
HX = 768
HY = HALF - HX
BLK = 40
GX = ("x", "zl", "c")
GX_GY = ("x", "zl", "c", "y", "zh")
BF = jnp.bfloat16
F32 = jnp.float32

momentum_keep = 0.9
learn_rate = 0.01


def ring(value, axis, step):
    return lax.ppermute(value, axis, [(i, (i + step) % 4) for i in range(4)])


def swap(value, axis):
    return lax.ppermute(value, axis, [(0, 1), (1, 0)])


def z_ring(value, step):
    at = lambda z: (z % 2) * 4 + z // 2
    return lax.ppermute(value, ("zl", "zh"), [(at(z), at((z + step) % 8)) for z in range(8)])


def ring_gather(piece, axis):
    h = piece.shape[0] // 2
    before = ring(piece, axis, 1)
    after = ring(piece, axis, -1)
    far_a = ring(before[:h], axis, 1)
    far_b = ring(after[h:], axis, -1)
    return [piece, after, far_a, far_b, before]


def ring_scatter_first(grads, axis):
    return ring(grads[0], axis, 1), ring(grads[1], axis, -1)


def ring_scatter_passed(a, b, grads):
    mid = grads[2]
    return tuple((mid[i].astype(F32) + v[0].astype(F32)).astype(BF) for i, v in enumerate((a, b)))


def ring_scatter_last(a, b, passed, grads, axis):
    own = grads[3]
    c, e = ring(passed[0], axis, 1), ring(passed[1], axis, -1)
    own_u = own[0].astype(F32) + c.astype(F32) + b[1].astype(F32)
    own_d = own[1].astype(F32) + a[1].astype(F32) + e.astype(F32)
    return jnp.concatenate([own_u, own_d], axis=1).astype(BF)


def direct_scatter(q, axis):
    r1 = ring(q[1], axis, 1)
    r3 = ring(q[3], axis, -1)
    r2 = ring(q[2], axis, 2)
    return q[0].astype(F32) + r1.astype(F32) + r2.astype(F32) + r3.astype(F32)


def direct_gather(piece, axis, index):
    before = ring(piece, axis, 1)
    after = ring(piece, axis, -1)
    far = ring(piece, axis, 2)
    relative = jnp.stack([piece, after, far, before])
    return rolled(relative, (4 - index) % 4)


def rolled(blocks, start):
    n = blocks.shape[0]
    return lax.dynamic_slice_in_dim(jnp.concatenate([blocks, blocks], axis=0), start, n, 0)


def direct_sum(value, axis):
    return value + ring(value, axis, 1) + ring(value, axis, -1) + ring(value, axis, 2)


def gelu_and_slope(v):
    t = jnp.tanh(0.7978845608 * (v + 0.044715 * v * v * v))
    half = 0.5 * (1.0 + t)
    slope = half + 0.5 * v * (1.0 - t * t) * (0.7978845608 * (1.0 + 0.134145 * v * v))
    return v * half, slope


def dot(left, right):
    return jnp.dot(left, right, preferred_element_type=F32)


def gradients_kernel(by_y, tok_refs, pieces, outs, scratch):
    plus, minus, mid, own = outs
    wu, wd, pg, hd, rows_in, columns_in, arrived = scratch
    places = (rows_in.at[0], rows_in.at[1], columns_in.at[0], columns_in.at[1])
    copies = [
        pltpu.make_async_copy(ref, place, arrived.at[i])
        for i, (ref, place) in enumerate(zip(tok_refs, places))
    ]

    @pl.when(pl.program_id(0) == 0)
    def _():
        for copy in copies:
            copy.start()

    count = len(pieces) // 2
    for group, whole in ((pieces[:count], wu), (pieces[count:], wd)):
        start = 0
        for piece in group:
            size = piece.shape[0]
            if by_y:
                for j in range(0, size, BLK):
                    dy, chunk = divmod((start + j) // BLK, 8)
                    at = (chunk * 4 + dy) * BLK
                    whole[at : at + BLK, :] = piece[j : j + BLK, :]
            else:
                whole[start : start + size, :] = piece[...]
            start += size

    @pl.when(pl.program_id(0) == 0)
    def _():
        for copy in copies[:2]:
            copy.wait()

    half = rows_in.shape[2]

    for core in range(2):
        for m in range(0, half, 256):
            v = dot(rows_in[core, 0, m : m + 256, :], wu[...])
            hidden_grad = dot(rows_in[core, 1, m : m + 256, :], wd[...])
            hidden, slope = gelu_and_slope(v)
            at = core * half + m
            hd[at : at + 256, :] = hidden.astype(BF)
            pg[at : at + 256, :] = (hidden_grad * slope).astype(BF)

    @pl.when(pl.program_id(0) == 0)
    def _():
        for copy in copies[2:]:
            copy.wait()

    q = D // 4
    up_to = ((own, 0), (mid, 0), (plus, 0), (minus, 1))
    down_to = ((own, 1), (plus, 1), (minus, 0), (mid, 1))
    for k in (2, 1, 3, 0):
        rows = slice(k * q, (k + 1) * q)
        for i, right, to in ((0, pg, up_to), (1, hd, down_to)):
            grad = dot(columns_in[0, i, rows, :], right[:half, :])
            grad += dot(columns_in[1, i, rows, :], right[half:, :])
            if by_y:
                for j in range(8):
                    dz, dy = divmod(j, 4)
                    out, slot = to[dy]
                    at = (k * 2 + dz) * BLK
                    out[slot, at : at + BLK, :] = grad[j * BLK : (j + 1) * BLK, :].astype(BF)
            else:
                out, slot = to[k]
                out[slot] = grad.astype(BF)


def gradients(pieces, features, by_y):
    h = pieces[0].shape[1] // 2
    tokens = 2 * features[0].shape[1]
    blocks = h // 256
    count = len(pieces)

    def body(*refs):
        tok_refs, refs = refs[:4], refs[4:]
        gradients_kernel(
            by_y, tok_refs, refs[: 2 * count], refs[2 * count : 2 * count + 4], refs[-7:]
        )

    at = lambda first: [
        pl.BlockSpec((p.shape[0], 256), lambda n, first=first: (0, n + first)) for p in pieces
    ]
    q = D // 4
    return pl.pallas_call(
        body,
        grid=(blocks,),
        in_specs=[pl.BlockSpec(memory_space=pl.ANY)] * 4 + at(0) + at(blocks),
        out_specs=[pl.BlockSpec((2, q, 256), lambda n: (0, 0, n))] * 4,
        out_shape=[jax.ShapeDtypeStruct((2, q, h), BF)] * 4,
        scratch_shapes=[pltpu.VMEM((D, 256), BF)] * 2
        + [pltpu.VMEM((tokens, 256), BF)] * 2
        + [pltpu.VMEM((2, 2, tokens // 2, D), BF), pltpu.VMEM((2, 2, D, tokens // 2), BF)]
        + [pltpu.SemaphoreType.DMA((4,))],
        compiler_params=pltpu.CompilerParams(vmem_limit_bytes=30 * 1024 * 1024),
        cost_estimate=pl.CostEstimate(
            flops=8 * tokens * D * h,
            bytes_accessed=2 * (4 * tokens * D + 4 * D * h),
            transcendentals=tokens * h,
        ),
        name="gradients_y" if by_y else "gradients_x",
    )(*features, *pieces, *pieces)


def turn_kernel(source, values, others, rows, columns):
    row = lax.broadcasted_iota(jnp.int32, (D, 256), 0)
    onehot = jnp.where(row == source[...], 1.0, 0.0).astype(BF)
    for i, left in enumerate((values, others)):
        turned = dot(left[...], onehot)
        rows[i] = turned.astype(BF)
        columns[i] = turned.T.astype(BF)


def turned(source, values, others):
    tokens = values.shape[0]
    whole = pl.BlockSpec((tokens, D), lambda n: (0, 0))
    return pl.pallas_call(
        turn_kernel,
        grid=(D // 256,),
        in_specs=[pl.BlockSpec((1, 256), lambda n: (0, n)), whole, whole],
        out_specs=[
            pl.BlockSpec((2, tokens, 256), lambda n: (0, 0, n)),
            pl.BlockSpec((2, 256, tokens), lambda n: (0, n, 0)),
        ],
        out_shape=[
            jax.ShapeDtypeStruct((2, tokens, D), BF),
            jax.ShapeDtypeStruct((2, D, tokens), BF),
        ],
        compiler_params=pltpu.CompilerParams(vmem_limit_bytes=20 * 1024 * 1024),
        cost_estimate=pl.CostEstimate(
            flops=4 * tokens * D * D, bytes_accessed=12 * tokens * D, transcendentals=0
        ),
        name="turn",
    )(source, values, others)


def table_lookup(positions, table):
    onehot = (positions[:, None] == jnp.arange(GRID, dtype=jnp.int32)[None, :]).astype(BF)
    return jnp.dot(onehot, table, preferred_element_type=F32)


def on_device(
    tokens,
    out_grad,
    segments,
    pos_rows,
    pos_cols,
    row_table,
    col_table,
    norm_gain,
    master_up,
    master_down,
    moment_up,
    moment_down,
):
    ix, iz, ic = lax.axis_index("x"), lax.axis_index("zl"), lax.axis_index("c")
    iy, ih = lax.axis_index("y"), lax.axis_index("zh")
    low_core = ic == 0

    up, down = master_up.astype(BF), master_down.astype(BF)

    def columns(k):
        u, d = up[:, k * HALF : (k + 1) * HALF], down[:, k * HALF : (k + 1) * HALF]
        return jnp.concatenate([u[:, :HX], d[:, :HX], u[:, HX:], d[:, HX:]], axis=1)

    lo, hi = columns(0), columns(1)
    mine = jnp.where(low_core, lo, hi)
    other = swap(jnp.where(low_core, hi, lo), "c")
    rows = jnp.concatenate(
        [jnp.where(low_core, mine, other), jnp.where(low_core, other, mine)], axis=0
    )
    rows = rolled(rows.reshape(4, BLK, 2 * HALF), iy).reshape(4 * BLK, 2 * HALF)

    tokens, out_grad, rows = lax.optimization_barrier((tokens, out_grad, rows))

    vx, vy = rows[:, : 2 * HX], rows[:BLK, 2 * HX :]

    def to_side(x_first, y_first):
        blocks = [vx[k * BLK : (k + 1) * BLK, x_first : x_first + HX] for k in range(4)]
        return jnp.concatenate([*blocks, vy[:, y_first : y_first + HY]], axis=1)

    low, high = z_ring(to_side(0, 0), 1), z_ring(to_side(HX, HY), -1)
    embedded = (
        tokens.astype(F32) + table_lookup(pos_rows, row_table) + table_lookup(pos_cols, col_table)
    )
    average = jnp.mean(embedded, axis=1, keepdims=True)
    centered = embedded - average
    variance = jnp.mean(centered * centered, axis=1, keepdims=True)
    normed = (centered * lax.rsqrt(variance + 1e-06) * norm_gain[None, :]).astype(BF)
    member = (segments[0][:, None] == jnp.arange(IMGS, dtype=jnp.int32)[None, :]).astype(F32)
    per_image = 1.0 / jnp.sum(member, axis=0)
    token_weight = jnp.sum(member * per_image[None, :], axis=1)
    weighted = (out_grad.astype(F32) * token_weight[:, None]).astype(BF)

    place = jnp.arange(D, dtype=jnp.int32)
    block, within = place // BLK, place % BLK
    source = ((ix + block // 8) % 4 * 2 + (iz + block // 4 % 2) % 2) * 4 + (iy + block % 4) % 4
    low, high, normed, weighted = lax.optimization_barrier((low, high, normed, weighted))
    row_form, column_form = turned((source * BLK + within)[None, :], normed, weighted)

    other_y = jnp.concatenate([low[:, 4 * HX :], high[:, 4 * HX :]], axis=1)
    other_x = [
        jnp.concatenate([part[:, k * HX : (k + 1) * HX] for part in (low, high)], axis=1)
        for k in range(4)
    ]
    wy = jnp.concatenate([vy, other_y], axis=0)
    before, after, far = ring(wy, "x", 1), ring(wy, "x", -1), ring(wy, "x", 2)
    wx = jnp.concatenate([vx, *other_x], axis=0)
    before, after, far, row_form, column_form = lax.optimization_barrier(
        (before, after, far, row_form, column_form)
    )
    wy = ring_gather(jnp.concatenate([wy, after, far, before], axis=0), "y")
    wx = ring_gather(wx, "x")

    features = [row_form, swap(row_form, "c"), column_form, swap(column_form, "c")]
    gy = gradients(wy, features, True)
    gx = gradients(wx, features, False)
    (a_x, b_x), (a_y, b_y) = ring_scatter_first(gx, "x"), ring_scatter_first(gy, "y")
    passed_x = ring_scatter_passed(a_x, b_x, gx)
    _, a_y, b_y = lax.optimization_barrier((passed_x, a_y, b_y))
    passed_y = ring_scatter_passed(a_y, b_y, gy)
    sx = ring_scatter_last(a_x, b_x, passed_x, gx, "x").reshape(2, 4, BLK, 2 * HX)
    sy = ring_scatter_last(a_y, b_y, passed_y, gy, "y").reshape(4, 2 * BLK, 2 * HY)
    sx = direct_scatter([sx[:, k].reshape(2 * BLK, 2 * HX) for k in range(4)], "y")
    sy = direct_scatter([sy[k] for k in range(4)], "x")
    both = jnp.concatenate([sx, sy], axis=1)
    both = both[:BLK] + swap(both[BLK:].astype(BF), "zl").astype(F32)
    parts = jnp.stack([both[:, k * 640 : (k + 1) * 640] for k in range(4)]).astype(BF)
    parts = rolled(parts, ih)
    share = direct_scatter([parts[k] for k in range(4)], "zh").astype(BF)

    gathered = direct_gather(share, "zh", ih)
    gathered = jnp.concatenate([gathered[k] for k in range(4)], axis=1)
    wide = gathered.astype(F32)
    squares = jnp.full((8, 128), jnp.sum(wide * wide), F32)
    squares = direct_sum(squares, "x")
    squares = squares + swap(squares, "zl")
    narrow = lambda value: lax.reduce_precision(value, 8, 7)
    second = squares - narrow(squares)
    third = second - narrow(second)
    row = lax.broadcasted_iota(jnp.int32, (8, 128), 0)
    terms = jnp.where(row == 0, squares, jnp.where(row == 1, second, jnp.where(row == 2, third, 0)))
    terms = jnp.broadcast_to(terms[:, :1], (8, 2 * HALF)).astype(BF)
    rows_of = lax.all_gather(jnp.concatenate([gathered, terms], axis=0), "y")
    terms = rows_of[:, BLK:].reshape(32, 2 * HALF)
    rows_of = rows_of[:, :BLK].reshape(4 * BLK, 2 * HALF)
    first, last = rows_of[: 2 * BLK], rows_of[2 * BLK :]
    keep = jnp.where(low_core, first, last)
    got = swap(jnp.concatenate([jnp.where(low_core, last, first), terms], axis=0), "c")
    total = terms[:, :128].astype(F32) + got[2 * BLK :, :128].astype(F32)
    total = jnp.sum(total, axis=0, keepdims=True)
    scale = lax.rsqrt(total[:, :1] / (2.0 * D * FF) + 1e-06)
    got = got[: 2 * BLK]
    lo, hi = jnp.where(low_core, keep, got), jnp.where(low_core, got, keep)

    def updated(start_x, start_y, master, moment):
        grad = jnp.concatenate(
            [
                part
                for half in (lo, hi)
                for part in (half[:, start_x : start_x + HX], half[:, start_y : start_y + HY])
            ],
            axis=1,
        ).astype(F32)
        new_moment = momentum_keep * moment + scale * grad
        return master - learn_rate * new_moment, new_moment

    new_up, new_moment_up = updated(0, 2 * HX, master_up, moment_up)
    new_down, new_moment_down = updated(HX, 2 * HX + HY, master_down, moment_down)
    return new_up, new_down, new_moment_up, new_moment_down


def solution(mesh):
    split = Mesh(mesh.devices.reshape(4, 2, 2, 4, 4), ("x", "zl", "c", "y", "zh"))
    return jax.shard_map(
        on_device,
        mesh=split,
        in_specs=(
            P(GX_GY, None),
            P(GX_GY, None),
            P(GX_GY, None),
            P(GX_GY),
            P(GX_GY),
            P(),
            P(),
            P(),
            P(GX, None),
            P(GX, None),
            P(GX, None),
            P(GX, None),
        ),
        out_specs=(P(GX, None), P(GX, None), P(GX, None), P(GX, None)),
        check_vma=False,
    )
```

```python
import jax
import jax.numpy as jnp
from jax import lax
from jax.experimental import pallas as pl
from jax.experimental.pallas import tpu as pltpu
from jax.sharding import Mesh
from jax.sharding import PartitionSpec as P

D = 1280
FF = 2560
GRID = 16
IMGS = 8
HALF = 1280
HX = 768
HY = HALF - HX
BLK = 40
GX = ("x", "zl", "c")
GX_GY = ("x", "zl", "c", "y", "zh")
BF = jnp.bfloat16
F32 = jnp.float32

momentum_keep = 0.9
learn_rate = 0.01


def ring(value, axis, step):
    return lax.ppermute(value, axis, [(i, (i + step) % 4) for i in range(4)])


def swap(value, axis):
    return lax.ppermute(value, axis, [(0, 1), (1, 0)])


def z_ring(value, step):
    at = lambda z: (z % 2) * 4 + z // 2
    return lax.ppermute(value, ("zl", "zh"), [(at(z), at((z + step) % 8)) for z in range(8)])


def ring_gather(piece, axis):
    h = piece.shape[0] // 2
    before = ring(piece, axis, 1)
    after = ring(piece, axis, -1)
    far_a = ring(before[:h], axis, 1)
    far_b = ring(after[h:], axis, -1)
    return [piece, after, far_a, far_b, before]


def ring_scatter_first(grads, axis):
    return ring(grads[0], axis, 1), ring(grads[1], axis, -1)


def ring_scatter_passed(a, b, grads):
    mid = grads[2]
    return tuple((mid[i].astype(F32) + v[0].astype(F32)).astype(BF) for i, v in enumerate((a, b)))


def ring_scatter_last(a, b, passed, grads, axis):
    own = grads[3]
    c, e = ring(passed[0], axis, 1), ring(passed[1], axis, -1)
    own_u = own[0].astype(F32) + c.astype(F32) + b[1].astype(F32)
    own_d = own[1].astype(F32) + a[1].astype(F32) + e.astype(F32)
    return jnp.concatenate([own_u, own_d], axis=1).astype(BF)


def direct_scatter(q, axis):
    r1 = ring(q[1], axis, 1)
    r3 = ring(q[3], axis, -1)
    r2 = ring(q[2], axis, 2)
    return q[0].astype(F32) + r1.astype(F32) + r2.astype(F32) + r3.astype(F32)


def direct_gather(piece, axis, index):
    before = ring(piece, axis, 1)
    after = ring(piece, axis, -1)
    far = ring(piece, axis, 2)
    relative = jnp.stack([piece, after, far, before])
    return rolled(relative, (4 - index) % 4)


def rolled(blocks, start):
    n = blocks.shape[0]
    return lax.dynamic_slice_in_dim(jnp.concatenate([blocks, blocks], axis=0), start, n, 0)


def direct_sum(value, axis):
    return value + ring(value, axis, 1) + ring(value, axis, -1) + ring(value, axis, 2)


def gelu_and_slope(v):
    t = jnp.tanh(0.7978845608 * (v + 0.044715 * v * v * v))
    half = 0.5 * (1.0 + t)
    slope = half + 0.5 * v * (1.0 - t * t) * (0.7978845608 * (1.0 + 0.134145 * v * v))
    return v * half, slope


def dot(left, right):
    return jnp.dot(left, right, preferred_element_type=F32)


def gradients_kernel(by_y, tok_refs, pieces, outs, scratch):
    plus, minus, mid, own = outs
    wu, wd, pg, hd, rows_in, columns_in, arrived = scratch
    places = (rows_in.at[0], rows_in.at[1], columns_in.at[0], columns_in.at[1])
    copies = [
        pltpu.make_async_copy(ref, place, arrived.at[i])
        for i, (ref, place) in enumerate(zip(tok_refs, places))
    ]

    @pl.when(pl.program_id(0) == 0)
    def _():
        for copy in copies:
            copy.start()

    count = len(pieces) // 2
    for group, whole in ((pieces[:count], wu), (pieces[count:], wd)):
        start = 0
        for piece in group:
            size = piece.shape[0]
            if by_y:
                for j in range(0, size, BLK):
                    dy, chunk = divmod((start + j) // BLK, 8)
                    at = (chunk * 4 + dy) * BLK
                    whole[at : at + BLK, :] = piece[j : j + BLK, :]
            else:
                whole[start : start + size, :] = piece[...]
            start += size

    @pl.when(pl.program_id(0) == 0)
    def _():
        for copy in copies[:2]:
            copy.wait()

    half = rows_in.shape[2]

    for core in range(2):
        for m in range(0, half, 256):
            v = dot(rows_in[core, 0, m : m + 256, :], wu[...])
            hidden_grad = dot(rows_in[core, 1, m : m + 256, :], wd[...])
            hidden, slope = gelu_and_slope(v)
            at = core * half + m
            hd[at : at + 256, :] = hidden.astype(BF)
            pg[at : at + 256, :] = (hidden_grad * slope).astype(BF)

    @pl.when(pl.program_id(0) == 0)
    def _():
        for copy in copies[2:]:
            copy.wait()

    q = D // 4
    up_to = ((own, 0), (mid, 0), (plus, 0), (minus, 1))
    down_to = ((own, 1), (plus, 1), (minus, 0), (mid, 1))
    for k in (2, 1, 3, 0):
        rows = slice(k * q, (k + 1) * q)
        for i, right, to in ((0, pg, up_to), (1, hd, down_to)):
            grad = dot(columns_in[0, i, rows, :], right[:half, :])
            grad += dot(columns_in[1, i, rows, :], right[half:, :])
            if by_y:
                for j in range(8):
                    dz, dy = divmod(j, 4)
                    out, slot = to[dy]
                    at = (k * 2 + dz) * BLK
                    out[slot, at : at + BLK, :] = grad[j * BLK : (j + 1) * BLK, :].astype(BF)
            else:
                out, slot = to[k]
                out[slot] = grad.astype(BF)


def gradients(pieces, features, by_y):
    h = pieces[0].shape[1] // 2
    tokens = 2 * features[0].shape[1]
    blocks = h // 256
    count = len(pieces)

    def body(*refs):
        tok_refs, refs = refs[:4], refs[4:]
        gradients_kernel(
            by_y, tok_refs, refs[: 2 * count], refs[2 * count : 2 * count + 4], refs[-7:]
        )

    at = lambda first: [
        pl.BlockSpec((p.shape[0], 256), lambda n, first=first: (0, n + first)) for p in pieces
    ]
    q = D // 4
    return pl.pallas_call(
        body,
        grid=(blocks,),
        in_specs=[pl.BlockSpec(memory_space=pl.ANY)] * 4 + at(0) + at(blocks),
        out_specs=[pl.BlockSpec((2, q, 256), lambda n: (0, 0, n))] * 4,
        out_shape=[jax.ShapeDtypeStruct((2, q, h), BF)] * 4,
        scratch_shapes=[pltpu.VMEM((D, 256), BF)] * 2
        + [pltpu.VMEM((tokens, 256), BF)] * 2
        + [pltpu.VMEM((2, 2, tokens // 2, D), BF), pltpu.VMEM((2, 2, D, tokens // 2), BF)]
        + [pltpu.SemaphoreType.DMA((4,))],
        compiler_params=pltpu.CompilerParams(vmem_limit_bytes=30 * 1024 * 1024),
        cost_estimate=pl.CostEstimate(
            flops=8 * tokens * D * h,
            bytes_accessed=2 * (4 * tokens * D + 4 * D * h),
            transcendentals=tokens * h,
        ),
        name="gradients_y" if by_y else "gradients_x",
    )(*features, *pieces, *pieces)


def turn_kernel(source, values, others, rows, columns):
    row = lax.broadcasted_iota(jnp.int32, (D, 256), 0)
    onehot = jnp.where(row == source[...], 1.0, 0.0).astype(BF)
    for i, left in enumerate((values, others)):
        turned = dot(left[...], onehot)
        rows[i] = turned.astype(BF)
        columns[i] = turned.T.astype(BF)


def turned(source, values, others):
    tokens = values.shape[0]
    whole = pl.BlockSpec((tokens, D), lambda n: (0, 0))
    return pl.pallas_call(
        turn_kernel,
        grid=(D // 256,),
        in_specs=[pl.BlockSpec((1, 256), lambda n: (0, n)), whole, whole],
        out_specs=[
            pl.BlockSpec((2, tokens, 256), lambda n: (0, 0, n)),
            pl.BlockSpec((2, 256, tokens), lambda n: (0, n, 0)),
        ],
        out_shape=[
            jax.ShapeDtypeStruct((2, tokens, D), BF),
            jax.ShapeDtypeStruct((2, D, tokens), BF),
        ],
        compiler_params=pltpu.CompilerParams(vmem_limit_bytes=20 * 1024 * 1024),
        cost_estimate=pl.CostEstimate(
            flops=4 * tokens * D * D, bytes_accessed=12 * tokens * D, transcendentals=0
        ),
        name="turn",
    )(source, values, others)


def table_lookup(positions, table):
    onehot = (positions[:, None] == jnp.arange(GRID, dtype=jnp.int32)[None, :]).astype(BF)
    return jnp.dot(onehot, table, preferred_element_type=F32)


def on_device(
    tokens,
    out_grad,
    segments,
    pos_rows,
    pos_cols,
    row_table,
    col_table,
    norm_gain,
    master_up,
    master_down,
    moment_up,
    moment_down,
):
    ix, iz, ic = lax.axis_index("x"), lax.axis_index("zl"), lax.axis_index("c")
    iy, ih = lax.axis_index("y"), lax.axis_index("zh")
    low_core = ic == 0

    up, down = master_up.astype(BF), master_down.astype(BF)

    def columns(k):
        u, d = up[:, k * HALF : (k + 1) * HALF], down[:, k * HALF : (k + 1) * HALF]
        return jnp.concatenate([u[:, :HX], d[:, :HX], u[:, HX:], d[:, HX:]], axis=1)

    lo, hi = columns(0), columns(1)
    mine = jnp.where(low_core, lo, hi)
    other = swap(jnp.where(low_core, hi, lo), "c")
    rows = jnp.concatenate(
        [jnp.where(low_core, mine, other), jnp.where(low_core, other, mine)], axis=0
    )
    rows = rolled(rows.reshape(4, BLK, 2 * HALF), iy).reshape(4 * BLK, 2 * HALF)

    tokens, out_grad, rows = lax.optimization_barrier((tokens, out_grad, rows))

    vx, vy = rows[:, : 2 * HX], rows[:BLK, 2 * HX :]

    def to_side(x_first, y_first):
        blocks = [vx[k * BLK : (k + 1) * BLK, x_first : x_first + HX] for k in range(4)]
        return jnp.concatenate([*blocks, vy[:, y_first : y_first + HY]], axis=1)

    low, high = z_ring(to_side(0, 0), 1), z_ring(to_side(HX, HY), -1)
    embedded = (
        tokens.astype(F32) + table_lookup(pos_rows, row_table) + table_lookup(pos_cols, col_table)
    )
    average = jnp.mean(embedded, axis=1, keepdims=True)
    centered = embedded - average
    variance = jnp.mean(centered * centered, axis=1, keepdims=True)
    normed = (centered * lax.rsqrt(variance + 1e-06) * norm_gain[None, :]).astype(BF)
    member = (segments[0][:, None] == jnp.arange(IMGS, dtype=jnp.int32)[None, :]).astype(F32)
    per_image = 1.0 / jnp.sum(member, axis=0)
    token_weight = jnp.sum(member * per_image[None, :], axis=1)
    weighted = (out_grad.astype(F32) * token_weight[:, None]).astype(BF)

    place = jnp.arange(D, dtype=jnp.int32)
    block, within = place // BLK, place % BLK
    source = ((ix + block // 8) % 4 * 2 + (iz + block // 4 % 2) % 2) * 4 + (iy + block % 4) % 4
    other_y = jnp.concatenate([low[:, 4 * HX :], high[:, 4 * HX :]], axis=1)
    other_x = [
        jnp.concatenate([part[:, k * HX : (k + 1) * HX] for part in (low, high)], axis=1)
        for k in range(4)
    ]
    wy = jnp.concatenate([vy, other_y], axis=0)
    before, after, far = ring(wy, "x", 1), ring(wy, "x", -1), ring(wy, "x", 2)
    wx = jnp.concatenate([vx, *other_x], axis=0)
    wx, before, after, far = lax.optimization_barrier((wx, before, after, far))
    wy = ring_gather(jnp.concatenate([wy, after, far, before], axis=0), "y")
    wx = ring_gather(wx, "x")

    row_form, column_form = turned((source * BLK + within)[None, :], normed, weighted)
    features = [row_form, swap(row_form, "c"), column_form, swap(column_form, "c")]
    gy = gradients(wy, features, True)
    gx = gradients(wx, features, False)
    (a_x, b_x), (a_y, b_y) = ring_scatter_first(gx, "x"), ring_scatter_first(gy, "y")
    passed_x = ring_scatter_passed(a_x, b_x, gx)
    _, a_y, b_y = lax.optimization_barrier((passed_x, a_y, b_y))
    passed_y = ring_scatter_passed(a_y, b_y, gy)
    sx = ring_scatter_last(a_x, b_x, passed_x, gx, "x").reshape(2, 4, BLK, 2 * HX)
    sy = ring_scatter_last(a_y, b_y, passed_y, gy, "y").reshape(4, 2 * BLK, 2 * HY)
    sx = direct_scatter([sx[:, k].reshape(2 * BLK, 2 * HX) for k in range(4)], "y")
    sy = direct_scatter([sy[k] for k in range(4)], "x")
    both = jnp.concatenate([sx, sy], axis=1)
    both = both[:BLK] + swap(both[BLK:].astype(BF), "zl").astype(F32)
    parts = jnp.stack([both[:, k * 640 : (k + 1) * 640] for k in range(4)]).astype(BF)
    parts = rolled(parts, ih)
    share = direct_scatter([parts[k] for k in range(4)], "zh").astype(BF)

    gathered = direct_gather(share, "zh", ih)
    gathered = jnp.concatenate([gathered[k] for k in range(4)], axis=1)
    wide = gathered.astype(F32)
    squares = jnp.full((8, 128), jnp.sum(wide * wide), F32)
    squares = direct_sum(squares, "x")
    squares = squares + swap(squares, "zl")
    narrow = lambda value: lax.reduce_precision(value, 8, 7)
    second = squares - narrow(squares)
    third = second - narrow(second)
    row = lax.broadcasted_iota(jnp.int32, (8, 128), 0)
    terms = jnp.where(row == 0, squares, jnp.where(row == 1, second, jnp.where(row == 2, third, 0)))
    terms = jnp.broadcast_to(terms[:, :1], (8, 2 * HALF)).astype(BF)
    rows_of = lax.all_gather(jnp.concatenate([gathered, terms], axis=0), "y")
    terms = rows_of[:, BLK:].reshape(32, 2 * HALF)
    rows_of = rows_of[:, :BLK].reshape(4 * BLK, 2 * HALF)
    first, last = rows_of[: 2 * BLK], rows_of[2 * BLK :]
    keep = jnp.where(low_core, first, last)
    got = swap(jnp.concatenate([jnp.where(low_core, last, first), terms], axis=0), "c")
    total = terms[:, :128].astype(F32) + got[2 * BLK :, :128].astype(F32)
    total = jnp.sum(total, axis=0, keepdims=True)
    scale = lax.rsqrt(total[:, :1] / (2.0 * D * FF) + 1e-06)
    got = got[: 2 * BLK]
    lo, hi = jnp.where(low_core, keep, got), jnp.where(low_core, got, keep)

    def updated(start_x, start_y, master, moment):
        grad = jnp.concatenate(
            [
                part
                for half in (lo, hi)
                for part in (half[:, start_x : start_x + HX], half[:, start_y : start_y + HY])
            ],
            axis=1,
        ).astype(F32)
        new_moment = momentum_keep * moment + scale * grad
        return master - learn_rate * new_moment, new_moment

    new_up, new_moment_up = updated(0, 2 * HX, master_up, moment_up)
    new_down, new_moment_down = updated(HX, 2 * HX + HY, master_down, moment_down)
    return new_up, new_down, new_moment_up, new_moment_down


def solution(mesh):
    split = Mesh(mesh.devices.reshape(4, 2, 2, 4, 4), ("x", "zl", "c", "y", "zh"))
    return jax.shard_map(
        on_device,
        mesh=split,
        in_specs=(
            P(GX_GY, None),
            P(GX_GY, None),
            P(GX_GY, None),
            P(GX_GY),
            P(GX_GY),
            P(),
            P(),
            P(),
            P(GX, None),
            P(GX, None),
            P(GX, None),
            P(GX, None),
        ),
        out_specs=(P(GX, None), P(GX, None), P(GX, None), P(GX, None)),
        check_vma=False,
    )
```
